16 devices in a mesh: dp: 2 (over y, z), tp: 8 (over x, core).
Axes of the slice: x: 4, y: 2, z: 1, core: 2. Of those that a mesh axis runs over, the one named last changes fastest.
The devices are a block of a 4x4x8 slice.
Arguments:
- x: bfloat16 [4096, 4096], P(('dp', 'tp')), parts along dimension 0
- w_gate: bfloat16 [4096, 10240], P(None, 'tp')
- w_up: bfloat16 [4096, 10240], P(None, 'tp')
- w_down: bfloat16 [10240, 4096], P('tp')
Outputs:
- output: bfloat16 [4096, 4096], P(('dp', 'tp')), parts along dimension 0
There are 2 independent parts. The reference program is written for one: setup_inputs(seed, part) draws one part's arguments, and reference() takes and returns one part's arrays. A program takes and returns all parts, laid end to end along the dimension named above; an argument that names none is the same for every part.
All inputs are finite; a program needn't handle non-finite values.
Results may differ from the reference program's by a relative error of at most 0.016.
Values are sent between devices in bfloat16 or wider.
A program may use at most 768 MiB of HBM per device.

```python
import jax
import jax.numpy as jnp

ROWS = 2048
D = 4096
FF = 10240


def setup_inputs(seed: int = 0, part: int = 0) -> dict:
    kx, kg, ku, kd = jax.random.split(jax.random.key(seed), 4)
    drawn = {
        "x": jax.random.normal(jax.random.fold_in(kx, part), (ROWS, D), jnp.float32),
        "w_gate": jax.random.normal(kg, (D, FF), jnp.float32) * D**-0.5,
        "w_up": jax.random.normal(ku, (D, FF), jnp.float32) * D**-0.5,
        "w_down": jax.random.normal(kd, (FF, D), jnp.float32) * FF**-0.5,
    }
    return {k: v.astype(jnp.bfloat16) for k, v in drawn.items()}


def reference(x, w_gate, w_up, w_down):
    gate = jnp.dot(x, w_gate, preferred_element_type=jnp.float32)
    up = jnp.dot(x, w_up, preferred_element_type=jnp.float32)
    hidden = (jax.nn.gelu(gate) * up).astype(jnp.bfloat16)
    return jnp.dot(hidden, w_down, preferred_element_type=jnp.float32).astype(jnp.bfloat16)
```

```python
import functools

import jax
import jax.numpy as jnp
from jax import lax
from jax.experimental import pallas as pl
from jax.experimental.pallas import tpu as pltpu
from jax.sharding import PartitionSpec as P

MESH = pl.DeviceIdType.MESH
FT = 256
NT = 512
OWN, NEAR, FAR, LAST = range(4)


def kernel(
    n, x, wg, wu, wd, y, xs, wgu, wds, h, rp, r3, stg,
    ag_send, ag_recv, d_send, d_recv, p_send, p_recv, r_send, r_recv, w_sem, wd_sem, x_sem, y_sem, credit,
):
    rows, depth = x.shape
    hidden = wg.shape[1]
    half, sub = rows // 2, rows // 4
    n_ft, n_nt = hidden // FT, depth // NT

    me = lax.axis_index("tp")
    core = lax.rem(me, 2)
    partner = me + 1 - 2 * core
    ahead = (lax.rem(me + 2, n), lax.rem(me + n - 2, n))

    def to(index):
        return dict(device_id={"tp": index}, device_id_type=MESH)

    barrier = pltpu.get_barrier_semaphore()
    for other in (*ahead, partner):
        pl.semaphore_signal(barrier, inc=1, **to(other))
    pl.semaphore_wait(barrier, 3)

    def piece(d, q):
        return pl.ds(d * half + q * sub, sub)

    def part_of(d):
        return pl.ds(d * half, half)

    def cols(t):
        return pl.ds(pl.multiple_of(t * NT, NT), NT)

    def gather(stage, d, q):
        src = {
            NEAR: x.at[piece(d, q)],
            FAR: xs.at[NEAR, core, piece(d, q)],
            LAST: x.at[piece(1 - d, q)],
        }[stage]
        return pltpu.make_async_remote_copy(
            src, xs.at[stage, core, piece(d, q)], ag_send.at[stage - 1, d, q], ag_recv.at[stage - 1, d, q], **to(ahead[d])
        )

    def share(stage, d, q):
        place = xs.at[stage, core, piece(d, q)]
        src = x.at[piece(d, q)] if stage == OWN else place
        return pltpu.make_async_remote_copy(src, place, d_send.at[stage, d, q], d_recv.at[stage, d, q], **to(partner))

    def trade(slot, src, t):
        return pltpu.make_async_remote_copy(
            src.at[:, cols(t)], rp.at[slot, :, cols(t)], p_send.at[slot, t], p_recv.at[slot, t], **to(partner)
        )

    def reduce(kind, d, t):
        src, dst = (
            (stg.at[part_of(1 - d), cols(t)], xs.at[OWN, 0, part_of(1 - d), cols(t)]),
            (xs.at[FAR, 1, part_of(d), cols(t)], xs.at[OWN, 1, part_of(1 - d), cols(t)]),
            (xs.at[LAST, 1, part_of(1 - d), cols(t)], r3.at[part_of(d), cols(t)]),
        )[kind]
        return pltpu.make_async_remote_copy(src, dst, r_send.at[kind, d, t], r_recv.at[kind, d, t], **to(ahead[d]))

    def load_x():
        return pltpu.make_async_copy(x, xs.at[OWN, core], x_sem)

    def load_w(j, which):
        src = (wg, wu)[which].at[:, pl.ds(pl.multiple_of(j * FT, FT), FT)]
        return pltpu.make_async_copy(src, wgu.at[j, :, pl.ds(which * FT, FT)], w_sem.at[which, j])

    def load_wd(t):
        return pltpu.make_async_copy(wd.at[:, cols(t)], wds.at[t], wd_sem.at[t])

    def store_y(t):
        return pltpu.make_async_copy(xs.at[NEAR, core, :, cols(t)], y.at[:, cols(t)], y_sem.at[t])

    pieces = [(d, q) for q in range(2) for d in range(2)]

    def up_stage(stage):
        @pl.loop(0, n_ft * 2)
        def _(i):
            j, m = i // 2, lax.rem(i, 2)
            if stage == OWN:

                @pl.when(m == 0)
                def _():
                    load_w(j, 0).wait()
                    load_w(j, 1).wait()

            both = jnp.dot(xs[stage, m], wgu[j], preferred_element_type=jnp.float32)
            value = (jax.nn.gelu(both[:, :FT]) * both[:, FT:]).astype(jnp.bfloat16)
            h[stage, m, :, pl.ds(pl.multiple_of(j * FT, FT), FT)] = value

    def term(stage, which, t):
        return jnp.dot(h[stage, which], wds[t], preferred_element_type=jnp.float32)

    def down_for_partner(stage, src, slot):
        @pl.loop(0, n_nt)
        def _(t):
            src[:, cols(t)] = term(stage, 1 - core, t).astype(jnp.bfloat16)
            trade(slot, src, t).start()

    def down_for_ring(stage, slot, dst, kind):
        @pl.loop(0, n_nt)
        def _(t):
            trade(slot, dst, t).wait_recv()
            total = term(stage, core, t) + rp[slot, :, cols(t)].astype(jnp.float32)
            if stage == LAST:
                for d in range(2):
                    reduce(1, d, t).wait_recv()
                total = total + xs[OWN, 1, :, cols(t)].astype(jnp.float32)
            dst[:, cols(t)] = total.astype(jnp.bfloat16)
            for d in range(2):
                reduce(kind, d, t).start()

    for d, q in pieces:
        gather(NEAR, d, q).start()
    load_x().start()
    for d, q in pieces:
        share(OWN, d, q).start()

    @pl.loop(0, n_ft)
    def _(j):
        load_w(j, 0).start()
        load_w(j, 1).start()

    @pl.loop(0, n_nt)
    def _(t):
        load_wd(t).start()

    load_x().wait()
    for d, q in pieces:
        share(OWN, d, q).wait_recv()
    up_stage(OWN)
    for other in ahead:
        pl.semaphore_signal(credit, inc=1, **to(other))

    for d, q in pieces:
        gather(NEAR, d, q).wait_recv()
        gather(FAR, d, q).start()
        share(NEAR, d, q).start()
    for d, q in pieces:
        gather(LAST, d, q).start()
    for d, q in pieces:
        share(NEAR, d, q).wait_recv()
    up_stage(NEAR)

    @pl.loop(0, n_nt)
    def _(t):
        load_wd(t).wait()

    spare = xs.at[NEAR, 1 - core]
    down_for_partner(NEAR, spare, 0)
    pl.semaphore_wait(credit, 2)
    down_for_ring(NEAR, 0, stg, 0)

    for d, q in pieces:
        gather(FAR, d, q).wait_recv()
        share(FAR, d, q).start()
    for d, q in pieces:
        share(FAR, d, q).wait()
    up_stage(FAR)
    down_for_partner(FAR, xs.at[FAR, 0], 1)
    down_for_ring(FAR, 1, xs.at[FAR, 1], 1)

    for d, q in pieces:
        gather(LAST, d, q).wait_recv()
        share(LAST, d, q).start()
    for d, q in pieces:
        share(LAST, d, q).wait()
    up_stage(LAST)

    @pl.loop(0, n_nt)
    def _(t):
        trade(0, spare, t).wait_send()
        trade(1, xs.at[FAR, 0], t).wait_send()

    down_for_partner(LAST, xs.at[LAST, 0], 0)
    down_for_partner(OWN, spare, 1)
    for d, q in pieces:
        share(OWN, d, q).wait_send()
        share(NEAR, d, q).wait_send()
        for stage in (NEAR, FAR, LAST):
            gather(stage, d, q).wait_send()
    down_for_ring(LAST, 0, xs.at[LAST, 1], 2)

    @pl.loop(0, n_nt)
    def _(t):
        trade(1, spare, t).wait_recv()
        total = term(OWN, core, t) + rp[1, :, cols(t)].astype(jnp.float32)
        for d in range(2):
            reduce(0, d, t).wait_recv()
        total = total + xs[OWN, 0, :, cols(t)].astype(jnp.float32)
        for d in range(2):
            reduce(2, d, t).wait_recv()
        total = total + r3[:, cols(t)].astype(jnp.float32)
        xs[NEAR, core, :, cols(t)] = total.astype(jnp.bfloat16)
        store_y(t).start()

    @pl.loop(0, n_nt)
    def _(t):
        trade(0, xs.at[LAST, 0], t).wait_send()
        trade(1, spare, t).wait_send()
        for kind in range(3):
            for d in range(2):
                reduce(kind, d, t).wait_send()
        store_y(t).wait()


def solution(mesh):
    n = mesh.shape["tp"]

    def step(x, w_gate, w_up, w_down):
        rows, depth = x.shape
        hidden = w_gate.shape[1]
        n_ft, n_nt = hidden // FT, depth // NT
        dma = pltpu.SemaphoreType.DMA
        any_space = pl.BlockSpec(memory_space=pl.ANY)
        flops = 6 * n * rows * depth * hidden
        return pl.pallas_call(
            functools.partial(kernel, n),
            out_shape=jax.ShapeDtypeStruct((rows, depth), jnp.bfloat16),
            in_specs=[any_space] * 4,
            out_specs=any_space,
            scratch_shapes=[
                pltpu.VMEM((4, 2, rows, depth), jnp.bfloat16),
                pltpu.VMEM((n_ft, depth, 2 * FT), jnp.bfloat16),
                pltpu.VMEM((n_nt, hidden, NT), jnp.bfloat16),
                pltpu.VMEM((4, 2, rows, hidden), jnp.bfloat16),
                pltpu.VMEM((2, rows, depth), jnp.bfloat16),
                pltpu.VMEM((rows, depth), jnp.bfloat16),
                pltpu.VMEM((rows, depth), jnp.bfloat16),
                dma((3, 2, 2)),
                dma((3, 2, 2)),
                dma((4, 2, 2)),
                dma((4, 2, 2)),
                dma((2, n_nt)),
                dma((2, n_nt)),
                dma((3, 2, n_nt)),
                dma((3, 2, n_nt)),
                dma((2, n_ft)),
                dma((n_nt,)),
                dma,
                dma((n_nt,)),
                pltpu.SemaphoreType.REGULAR,
            ],
            compiler_params=pltpu.CompilerParams(
                collective_id=0, has_side_effects=True, vmem_limit_bytes=67043328
            ),
            cost_estimate=pl.CostEstimate(flops=flops, bytes_accessed=6 * depth * hidden, transcendentals=0),
        )(x, w_gate, w_up, w_down)

    return jax.shard_map(
        step,
        mesh=mesh,
        in_specs=(P(("dp", "tp"), None), P(None, "tp"), P(None, "tp"), P("tp", None)),
        out_specs=P(("dp", "tp"), None),
        check_vma=False,
    )
```

```python
import functools

import jax
import jax.numpy as jnp
from jax import lax
from jax.experimental import pallas as pl
from jax.experimental.pallas import tpu as pltpu
from jax.sharding import PartitionSpec as P

MESH = pl.DeviceIdType.MESH
FT = 256
NT = 512
CHUNKS = ((8,), (4, 4), (4, 2, 1, 1))
OWN, NEAR, FAR, LAST = range(4)


def kernel(
    n, x, wg, wu, wd, y, xs, wgu, wds, h, rp, r3, stg,
    ag_send, ag_recv, d_send, d_recv, p_send, p_recv, r_send, r_recv, w_sem, wd_sem, x_sem, credit,
):
    rows, depth = x.shape
    hidden = wg.shape[1]
    half, sub = rows // 2, rows // 4
    n_ft, n_nt = hidden // FT, depth // NT

    me = lax.axis_index("tp")
    core = lax.rem(me, 2)
    partner = me + 1 - 2 * core
    ahead = (lax.rem(me + 2, n), lax.rem(me + n - 2, n))

    def to(index):
        return dict(device_id={"tp": index}, device_id_type=MESH)

    barrier = pltpu.get_barrier_semaphore()
    for other in (*ahead, partner):
        pl.semaphore_signal(barrier, inc=1, **to(other))
    pl.semaphore_wait(barrier, 3)

    def piece(d, q):
        return pl.ds(d * half + q * sub, sub)

    def part_of(d):
        return pl.ds(d * half, half)

    def cols(t):
        return pl.ds(pl.multiple_of(t * NT, NT), NT)

    def gather(stage, d, q=0):
        place = part_of(d) if stage == LAST else piece(d, q)
        src = {
            NEAR: x.at[place],
            FAR: xs.at[NEAR, core, place],
            LAST: x.at[part_of(1 - d)],
        }[stage]
        return pltpu.make_async_remote_copy(
            src, xs.at[stage, core, place], ag_send.at[stage - 1, d, q], ag_recv.at[stage - 1, d, q], **to(ahead[d])
        )

    def share(stage, d, q):
        place = xs.at[stage, core, piece(d, q)]
        src = x.at[piece(d, q)] if stage == OWN else place
        return pltpu.make_async_remote_copy(src, place, d_send.at[stage, d, q], d_recv.at[stage, d, q], **to(partner))

    def trade(slot, src, t):
        return pltpu.make_async_remote_copy(
            src.at[:, cols(t)], rp.at[slot, :, cols(t)], p_send.at[slot, t], p_recv.at[slot, t], **to(partner)
        )

    def reduce(kind, d, i):
        first = sum(CHUNKS[kind][:i])
        some = pl.ds(first * NT, CHUNKS[kind][i] * NT)
        src, dst = (
            (stg.at[part_of(1 - d), some], xs.at[OWN, 0, part_of(1 - d), some]),
            (xs.at[FAR, 1, part_of(d), some], xs.at[OWN, 1, part_of(1 - d), some]),
            (xs.at[LAST, 1, part_of(1 - d), some], r3.at[part_of(d), some]),
        )[kind]
        return pltpu.make_async_remote_copy(src, dst, r_send.at[kind, d, i], r_recv.at[kind, d, i], **to(ahead[d]))

    def await_sums(kind, t):
        for i in range(len(CHUNKS[kind])):

            @pl.when(t == sum(CHUNKS[kind][:i]))
            def _(i=i):
                for d in range(2):
                    reduce(kind, d, i).wait_recv()

    def send_sums(kind, t):
        for i in range(len(CHUNKS[kind])):

            @pl.when(t == sum(CHUNKS[kind][: i + 1]) - 1)
            def _(i=i):
                for d in range(2):
                    reduce(kind, d, i).start()

    def load_x():
        return pltpu.make_async_copy(x, xs.at[OWN, core], x_sem)

    def load_w(j, which):
        src = (wg, wu)[which].at[:, pl.ds(pl.multiple_of(j * FT, FT), FT)]
        return pltpu.make_async_copy(src, wgu.at[j, :, pl.ds(which * FT, FT)], w_sem.at[which, j])

    def load_wd(t):
        return pltpu.make_async_copy(wd.at[:, cols(t)], wds.at[t], wd_sem.at[t])

    pieces = [(d, q) for q in range(2) for d in range(2)]

    def up_stage(stage):
        @pl.loop(0, n_ft * 2)
        def _(i):
            j, m = i // 2, lax.rem(i, 2)
            if stage == OWN:

                @pl.when(m == 0)
                def _():
                    load_w(j, 0).wait()
                    load_w(j, 1).wait()

            both = jnp.dot(xs[stage, m], wgu[j], preferred_element_type=jnp.float32)
            value = (jax.nn.gelu(both[:, :FT]) * both[:, FT:]).astype(jnp.bfloat16)
            h[stage, m, :, pl.ds(pl.multiple_of(j * FT, FT), FT)] = value

    def term(stage, which, t):
        return jnp.dot(h[stage, which], wds[t], preferred_element_type=jnp.float32)

    def down_for_partner(stage, src, slot):
        @pl.loop(0, n_nt)
        def _(t):
            src[:, cols(t)] = term(stage, 1 - core, t).astype(jnp.bfloat16)
            trade(slot, src, t).start()

    def down_for_ring(stage, slot, dst, kind):
        @pl.loop(0, n_nt)
        def _(t):
            trade(slot, dst, t).wait_recv()
            total = term(stage, core, t) + rp[slot, :, cols(t)].astype(jnp.float32)
            if stage == LAST:
                await_sums(1, t)
                total = total + xs[OWN, 1, :, cols(t)].astype(jnp.float32)
            dst[:, cols(t)] = total.astype(jnp.bfloat16)
            send_sums(kind, t)

    for d, q in pieces:
        gather(NEAR, d, q).start()
    load_x().start()
    for d, q in pieces:
        share(OWN, d, q).start()

    @pl.loop(0, n_ft)
    def _(j):
        load_w(j, 0).start()
        load_w(j, 1).start()

    @pl.loop(0, n_nt)
    def _(t):
        load_wd(t).start()

    load_x().wait()
    for d, q in pieces:
        share(OWN, d, q).wait_recv()
    up_stage(OWN)
    for other in ahead:
        pl.semaphore_signal(credit, inc=1, **to(other))

    for d, q in pieces:
        gather(NEAR, d, q).wait_recv()
        gather(FAR, d, q).start()
        share(NEAR, d, q).start()
    for d in range(2):
        gather(LAST, d).start()
    for d, q in pieces:
        share(NEAR, d, q).wait_recv()
    up_stage(NEAR)

    @pl.loop(0, n_nt)
    def _(t):
        load_wd(t).wait()

    spare = xs.at[NEAR, 1 - core]
    down_for_partner(NEAR, spare, 0)
    pl.semaphore_wait(credit, 2)
    down_for_ring(NEAR, 0, stg, 0)

    for d, q in pieces:
        gather(FAR, d, q).wait_recv()
        share(FAR, d, q).start()
    for d, q in pieces:
        share(FAR, d, q).wait()
    up_stage(FAR)
    down_for_partner(FAR, xs.at[FAR, 0], 1)
    down_for_ring(FAR, 1, xs.at[FAR, 1], 1)

    for d in range(2):
        gather(LAST, d).wait_recv()
    for d, q in pieces:
        share(LAST, d, q).start()
    for d, q in pieces:
        share(LAST, d, q).wait()
    up_stage(LAST)

    @pl.loop(0, n_nt)
    def _(t):
        trade(0, spare, t).wait_send()
        trade(1, xs.at[FAR, 0], t).wait_send()

    down_for_partner(LAST, xs.at[LAST, 0], 0)
    down_for_partner(OWN, spare, 1)
    for d, q in pieces:
        share(OWN, d, q).wait_send()
        share(NEAR, d, q).wait_send()
        gather(NEAR, d, q).wait_send()
        gather(FAR, d, q).wait_send()
    for d in range(2):
        gather(LAST, d).wait_send()
    down_for_ring(LAST, 0, xs.at[LAST, 1], 2)

    @pl.loop(0, n_nt)
    def _(t):
        trade(1, spare, t).wait_recv()
        total = term(OWN, core, t) + rp[1, :, cols(t)].astype(jnp.float32)
        await_sums(0, t)
        total = total + xs[OWN, 0, :, cols(t)].astype(jnp.float32)
        await_sums(2, t)
        total = total + r3[:, cols(t)].astype(jnp.float32)
        y[:, cols(t)] = total.astype(jnp.bfloat16)

    @pl.loop(0, n_nt)
    def _(t):
        trade(0, xs.at[LAST, 0], t).wait_send()
        trade(1, spare, t).wait_send()

    for kind in range(3):
        for i in range(len(CHUNKS[kind])):
            for d in range(2):
                reduce(kind, d, i).wait_send()


def solution(mesh):
    n = mesh.shape["tp"]

    def step(x, w_gate, w_up, w_down):
        rows, depth = x.shape
        hidden = w_gate.shape[1]
        n_ft, n_nt = hidden // FT, depth // NT
        dma = pltpu.SemaphoreType.DMA
        any_space = pl.BlockSpec(memory_space=pl.ANY)
        flops = 6 * n * rows * depth * hidden
        return pl.pallas_call(
            functools.partial(kernel, n),
            out_shape=pltpu.VMEM((rows, depth), jnp.bfloat16),
            in_specs=[any_space] * 4,
            out_specs=pl.BlockSpec(memory_space=pltpu.VMEM),
            scratch_shapes=[
                pltpu.VMEM((4, 2, rows, depth), jnp.bfloat16),
                pltpu.VMEM((n_ft, depth, 2 * FT), jnp.bfloat16),
                pltpu.VMEM((n_nt, hidden, NT), jnp.bfloat16),
                pltpu.VMEM((4, 2, rows, hidden), jnp.bfloat16),
                pltpu.VMEM((2, rows, depth), jnp.bfloat16),
                pltpu.VMEM((rows, depth), jnp.bfloat16),
                pltpu.VMEM((rows, depth), jnp.bfloat16),
                dma((3, 2, 2)),
                dma((3, 2, 2)),
                dma((4, 2, 2)),
                dma((4, 2, 2)),
                dma((2, n_nt)),
                dma((2, n_nt)),
                dma((3, 2, len(CHUNKS[2]))),
                dma((3, 2, len(CHUNKS[2]))),
                dma((2, n_ft)),
                dma((n_nt,)),
                dma,
                pltpu.SemaphoreType.REGULAR,
            ],
            compiler_params=pltpu.CompilerParams(
                collective_id=0, has_side_effects=True, vmem_limit_bytes=61 * 2**20
            ),
            cost_estimate=pl.CostEstimate(flops=flops, bytes_accessed=6 * depth * hidden, transcendentals=0),
        )(x, w_gate, w_up, w_down)
    return jax.shard_map(
        step,
        mesh=mesh,
        in_specs=(P(("dp", "tp"), None), P(None, "tp"), P(None, "tp"), P("tp", None)),
        out_specs=P(("dp", "tp"), None),
        check_vma=False,
    )
```

```python
import functools

import jax
import jax.numpy as jnp
from jax import lax
from jax.experimental import pallas as pl
from jax.experimental.pallas import tpu as pltpu
from jax.sharding import PartitionSpec as P

MESH = pl.DeviceIdType.MESH
FT = 256
NT = 512
FAR_PARTS = (4, 4)
LAST_PARTS = (4, 3, 1)
OWN, NEAR, FAR, LAST = range(4)


def kernel(
    n, x, wg, wu, wd, y, xs, wgu, wds, h, rp, rf, stg,
    g_send, g_recv, d_send, d_recv, p_send, p_recv, n_send, n_recv, f_send, f_recv, l_send, l_recv,
    w_sem, wd_sem, x_sem, ready, credit, late_credit,
):
    rows, depth = x.shape
    hidden = wg.shape[1]
    half = rows // 2
    n_ft, n_nt = hidden // FT, depth // NT

    me = lax.axis_index("tp")
    core = lax.rem(me, 2)
    other = 1 - core
    way = other
    partner = me + 1 - 2 * core
    ahead = lax.rem(me + 4 * core - 2 + n, n)
    behind = lax.rem(me + 2 - 4 * core + n, n)
    beside = ahead + 1 - 2 * core

    def to(index):
        return dict(device_id={"tp": index}, device_id_type=MESH)

    def block(i):
        return pl.ds(pl.multiple_of(i * half, half), half)

    def cols(t, steps=1):
        return pl.ds(pl.multiple_of(t * NT, NT), steps * NT)

    def gather(stage, i):
        origin = (core, other)[i]
        part = block(1 - way if stage == LAST else way)
        src = xs.at[NEAR, way, block(origin)] if stage == FAR else (x.at[part], xs.at[OWN, other, part])[i]
        dst = xs.at[stage, way, block(origin)]
        return pltpu.make_async_remote_copy(src, dst, g_send.at[stage, i], g_recv.at[stage, i], **to(ahead))

    def share(stage, i):
        if stage == OWN:
            part = block((core, other)[i])
            src, dst = x.at[part], xs.at[OWN, core, part]
        else:
            src = dst = xs.at[stage, way, block((core, other)[i])]
        return pltpu.make_async_remote_copy(src, dst, d_send.at[stage, i], d_recv.at[stage, i], **to(partner))

    def trade(slot, src, t):
        return pltpu.make_async_remote_copy(
            src.at[:, cols(t)], rp.at[slot, :, cols(t)], p_send.at[slot, t], p_recv.at[slot, t], **to(partner)
        )

    def near_sum(owner, sent=None):
        sent = way if sent is None else sent
        return pltpu.make_async_remote_copy(
            stg.at[block(owner)], xs.at[OWN, owner, block(1 - sent)],
            n_send.at[owner], n_recv.at[sent], **to(ahead - core + owner),
        )

    def far_sum(i):
        some = pl.ds(sum(FAR_PARTS[:i]) * NT, FAR_PARTS[i] * NT)
        return pltpu.make_async_remote_copy(xs.at[FAR, 1, :, some], rf.at[:, some], f_send.at[i], f_recv.at[i], **to(ahead))

    def last_sum(i, owner, sent=None):
        sent = way if sent is None else sent
        some = pl.ds(sum(LAST_PARTS[:i]) * NT, LAST_PARTS[i] * NT)
        return pltpu.make_async_remote_copy(
            xs.at[LAST, 1, block(owner), some], xs.at[OWN, 1 - owner, block(sent), some],
            l_send.at[i, owner], l_recv.at[i, sent], **to(ahead - core + owner),
        )

    def at_start(parts, t, act):
        for i in range(len(parts)):
            pl.when(t == sum(parts[:i]))(functools.partial(act, i))

    def at_end(parts, t, act):
        for i in range(len(parts)):
            pl.when(t == sum(parts[: i + 1]) - 1)(functools.partial(act, i))

    def load_x():
        return pltpu.make_async_copy(x, xs.at[OWN, core], x_sem)

    def load_w(j, which):
        src = (wg, wu)[which].at[:, pl.ds(pl.multiple_of(j * FT, FT), FT)]
        return pltpu.make_async_copy(src, wgu.at[j, :, pl.ds(which * FT, FT)], w_sem.at[which, j])

    def load_wd(t):
        return pltpu.make_async_copy(wd.at[:, cols(t)], wds.at[t], wd_sem.at[t])

    def up_stage(stage):
        @pl.loop(0, n_ft * 2)
        def _(i):
            j, m = i // 2, lax.rem(i, 2)
            if stage == OWN:

                @pl.when(m == 0)
                def _():
                    load_w(j, 0).wait()
                    load_w(j, 1).wait()

            both = jnp.dot(xs[stage, m], wgu[j], preferred_element_type=jnp.float32)
            value = (jax.nn.gelu(both[:, :FT]) * both[:, FT:]).astype(jnp.bfloat16)
            h[stage, m, :, pl.ds(pl.multiple_of(j * FT, FT), FT)] = value

    def term(stage, which, t):
        return jnp.dot(h[stage, which], wds[t], preferred_element_type=jnp.float32)

    def down_for_partner(stage, which, src, slot):
        @pl.loop(0, n_nt)
        def _(t):
            src[:, cols(t)] = term(stage, which, t).astype(jnp.bfloat16)
            trade(slot, src, t).start()

    def chip_sum(stage, which, slot, t):
        trade(slot, spare, t).wait_recv()
        return term(stage, which, t) + rp[slot, :, cols(t)].astype(jnp.float32)

    spare = xs.at[NEAR, core]

    barrier = pltpu.get_barrier_semaphore()
    pl.semaphore_signal(barrier, inc=1, **to(behind))

    @pl.when(core == 1)
    def _():
        pl.semaphore_signal(barrier, inc=1, **to(partner))
        pl.semaphore_wait(barrier, 1)

    @pl.when(core == 0)
    def _():
        pl.semaphore_wait(barrier, 2)

    gather(NEAR, 0).start()
    load_x().start()

    @pl.when(core == 0)
    def _():
        pl.semaphore_signal(ready, inc=1, **to(partner))

    @pl.loop(0, n_ft)
    def _(j):
        load_w(j, 0).start()
        load_w(j, 1).start()

    @pl.loop(0, n_nt)
    def _(t):
        load_wd(t).start()

    @pl.when(core == 1)
    def _():
        pl.semaphore_wait(ready, 1)

    for i in range(2):
        share(OWN, i).start()
    share(OWN, 0).wait_recv()
    share(OWN, 1).wait_recv()
    gather(NEAR, 1).start()
    load_x().wait()
    up_stage(OWN)

    for i in range(2):
        gather(NEAR, i).wait_recv()
        gather(FAR, i).start()
        share(NEAR, i).start()
    for i in range(2):
        gather(LAST, i).start()
    for i in range(2):
        share(NEAR, i).wait_recv()
    for writer in (behind, beside):
        pl.semaphore_signal(credit, inc=1, **to(writer))
    up_stage(NEAR)

    @pl.loop(0, n_nt)
    def _(t):
        load_wd(t).wait()

    down_for_partner(NEAR, other, spare, 0)

    @pl.loop(0, n_nt)
    def _(t):
        stg[:, cols(t)] = chip_sum(NEAR, core, 0, t).astype(jnp.bfloat16)

    pl.semaphore_wait(credit, 2)
    for owner in range(2):
        near_sum(owner).start()

    for i in range(2):
        gather(FAR, i).wait_recv()
        share(FAR, i).start()
    for i in range(2):
        share(FAR, i).wait()
    up_stage(FAR)
    down_for_partner(FAR, core, xs.at[FAR, 0], 1)

    @pl.loop(0, n_nt)
    def _(t):
        xs[FAR, 1, :, cols(t)] = chip_sum(FAR, other, 1, t).astype(jnp.bfloat16)
        at_end(FAR_PARTS, t, lambda i: far_sum(i).start())

    for i in range(2):
        gather(LAST, i).wait_recv()
        share(LAST, i).start()
    for i in range(2):
        gather(LAST, i).wait_send()
        gather(NEAR, i).wait_send()
    for writer in (behind, beside):
        pl.semaphore_signal(late_credit, inc=1, **to(writer))
    for i in range(2):
        share(LAST, i).wait()
    up_stage(LAST)

    @pl.loop(0, n_nt)
    def _(t):
        trade(0, spare, t).wait_send()
        trade(1, xs.at[FAR, 0], t).wait_send()

    down_for_partner(LAST, other, xs.at[LAST, 0], 0)
    down_for_partner(OWN, other, spare, 1)
    pl.semaphore_wait(late_credit, 2)

    def send_last(i):
        for owner in range(2):
            last_sum(i, owner).start()

    @pl.loop(0, n_nt)
    def _(t):
        total = chip_sum(LAST, core, 0, t)
        at_start(FAR_PARTS, t, lambda i: far_sum(i).wait_recv())
        total = total + rf[:, cols(t)].astype(jnp.float32)
        xs[LAST, 1, :, cols(t)] = total.astype(jnp.bfloat16)
        at_end(LAST_PARTS, t, send_last)

    for sent in range(2):
        near_sum(core, sent).wait_recv()

    def await_last(i):
        for sent in range(2):
            last_sum(i, core, sent).wait_recv()

    @pl.loop(0, n_nt)
    def _(t):
        total = chip_sum(OWN, core, 1, t) + xs[OWN, core, :, cols(t)].astype(jnp.float32)
        at_start(LAST_PARTS, t, await_last)
        total = total + xs[OWN, other, :, cols(t)].astype(jnp.float32)
        y[:, cols(t)] = total.astype(jnp.bfloat16)

    @pl.loop(0, n_nt)
    def _(t):
        trade(0, xs.at[LAST, 0], t).wait_send()
        trade(1, spare, t).wait_send()

    for i in range(2):
        gather(FAR, i).wait_send()
        share(OWN, i).wait_send()
        share(NEAR, i).wait_send()
        near_sum(i).wait_send()
    for i in range(len(FAR_PARTS)):
        far_sum(i).wait_send()
    for i in range(len(LAST_PARTS)):
        for owner in range(2):
            last_sum(i, owner).wait_send()


def solution(mesh):
    n = mesh.shape["tp"]

    def step(x, w_gate, w_up, w_down):
        rows, depth = x.shape
        hidden = w_gate.shape[1]
        n_ft, n_nt = hidden // FT, depth // NT
        dma, plain = pltpu.SemaphoreType.DMA, pltpu.SemaphoreType.REGULAR
        any_space = pl.BlockSpec(memory_space=pl.ANY)
        return pl.pallas_call(
            functools.partial(kernel, n),
            out_shape=pltpu.VMEM((rows, depth), jnp.bfloat16),
            in_specs=[any_space] * 4,
            out_specs=pl.BlockSpec(memory_space=pltpu.VMEM),
            scratch_shapes=[
                pltpu.VMEM((4, 2, rows, depth), jnp.bfloat16),
                pltpu.VMEM((n_ft, depth, 2 * FT), jnp.bfloat16),
                pltpu.VMEM((n_nt, hidden, NT), jnp.bfloat16),
                pltpu.VMEM((4, 2, rows, hidden), jnp.bfloat16),
                pltpu.VMEM((2, rows, depth), jnp.bfloat16),
                pltpu.VMEM((rows, depth), jnp.bfloat16),
                pltpu.VMEM((rows, depth), jnp.bfloat16),
                dma((4, 2)),
                dma((4, 2)),
                dma((4, 2)),
                dma((4, 2)),
                dma((2, n_nt)),
                dma((2, n_nt)),
                dma((2,)),
                dma((2,)),
                dma((len(FAR_PARTS),)),
                dma((len(FAR_PARTS),)),
                dma((len(LAST_PARTS), 2)),
                dma((len(LAST_PARTS), 2)),
                dma((2, n_ft)),
                dma((n_nt,)),
                dma,
                plain,
                plain,
                plain,
            ],
            compiler_params=pltpu.CompilerParams(
                collective_id=0, has_side_effects=True, vmem_limit_bytes=61 * 2**20
            ),
            cost_estimate=pl.CostEstimate(
                flops=6 * n * rows * depth * hidden, bytes_accessed=6 * depth * hidden, transcendentals=0
            ),
        )(x, w_gate, w_up, w_down)

    return jax.shard_map(
        step,
        mesh=mesh,
        in_specs=(P(("dp", "tp"), None), P(None, "tp"), P(None, "tp"), P("tp", None)),
        out_specs=P(("dp", "tp"), None),
        check_vma=False,
    )
```

```python
import functools

import jax
import jax.numpy as jnp
from jax import lax
from jax.experimental import pallas as pl
from jax.experimental.pallas import tpu as pltpu
from jax.sharding import PartitionSpec as P

MESH = pl.DeviceIdType.MESH
FT = 256
NT = 512
FAR_PARTS = (4, 4)
LAST_PARTS = (4, 3, 1)
OWN, NEAR, FAR, LAST = range(4)


def kernel(
    n, x, wg, wu, wd, y, xs, wgu, wds, h, rp, rf, stg,
    g_send, g_recv, d_send, d_recv, p_send, p_recv, n_send, n_recv, f_send, f_recv, l_send, l_recv,
    w_sem, wd_sem, x_sem, ready, credit, late_credit,
):
    rows, depth = x.shape
    hidden = wg.shape[1]
    half = rows // 2
    n_ft, n_nt = hidden // FT, depth // NT

    me = lax.axis_index("tp")
    core = lax.rem(me, 2)
    other = 1 - core
    way = other
    partner = me + 1 - 2 * core
    ahead = lax.rem(me + 4 * core - 2 + n, n)
    behind = lax.rem(me + 2 - 4 * core + n, n)
    beside = ahead + 1 - 2 * core

    def to(index):
        return dict(device_id={"tp": index}, device_id_type=MESH)

    def block(i):
        return pl.ds(pl.multiple_of(i * half, half), half)

    def cols(t, steps=1):
        return pl.ds(pl.multiple_of(t * NT, NT), steps * NT)

    def gather(stage, i):
        origin = (core, other)[i]
        part = block(1 - way if stage == LAST else way)
        src = xs.at[NEAR, way, block(origin)] if stage == FAR else (x.at[part], xs.at[OWN, other, part])[i]
        dst = xs.at[stage, way, block(origin)]
        return pltpu.make_async_remote_copy(src, dst, g_send.at[stage, i], g_recv.at[stage, i], **to(ahead))

    def share(stage, i):
        if stage == OWN:
            part = block((core, other)[i])
            src, dst = x.at[part], xs.at[OWN, core, part]
        else:
            src = dst = xs.at[stage, way, block((core, other)[i])]
        return pltpu.make_async_remote_copy(src, dst, d_send.at[stage, i], d_recv.at[stage, i], **to(partner))

    def trade(slot, src, t):
        return pltpu.make_async_remote_copy(
            src.at[:, cols(t)], rp.at[slot, :, cols(t)], p_send.at[slot, t], p_recv.at[slot, t], **to(partner)
        )

    def near_sum(owner, sent=None):
        sent = way if sent is None else sent
        return pltpu.make_async_remote_copy(
            stg.at[block(owner)], xs.at[OWN, owner, block(1 - sent)],
            n_send.at[owner], n_recv.at[sent], **to(ahead - core + owner),
        )

    def far_sum(i):
        some = pl.ds(sum(FAR_PARTS[:i]) * NT, FAR_PARTS[i] * NT)
        return pltpu.make_async_remote_copy(xs.at[FAR, 1, :, some], rf.at[:, some], f_send.at[i], f_recv.at[i], **to(ahead))

    def last_sum(i, owner, sent=None):
        sent = way if sent is None else sent
        some = pl.ds(sum(LAST_PARTS[:i]) * NT, LAST_PARTS[i] * NT)
        return pltpu.make_async_remote_copy(
            xs.at[LAST, 1, block(owner), some], xs.at[OWN, 1 - owner, block(sent), some],
            l_send.at[i, owner], l_recv.at[i, sent], **to(ahead - core + owner),
        )

    def at_start(parts, t, act):
        for i in range(len(parts)):
            pl.when(t == sum(parts[:i]))(functools.partial(act, i))

    def at_end(parts, t, act):
        for i in range(len(parts)):
            pl.when(t == sum(parts[: i + 1]) - 1)(functools.partial(act, i))

    def load_x():
        return pltpu.make_async_copy(x, xs.at[OWN, core], x_sem)

    def load_w(j, which):
        src = (wg, wu)[which].at[:, pl.ds(pl.multiple_of(j * FT, FT), FT)]
        return pltpu.make_async_copy(src, wgu.at[j, :, pl.ds(which * FT, FT)], w_sem.at[which, j])

    def load_wd(t):
        return pltpu.make_async_copy(wd.at[:, cols(t)], wds.at[t], wd_sem.at[t])

    def up_stage(stage):
        @pl.loop(0, n_ft * 2)
        def _(i):
            j, m = i // 2, lax.rem(i, 2)
            if stage == OWN:

                @pl.when(m == 0)
                def _():
                    load_w(j, 0).wait()
                    load_w(j, 1).wait()

            both = jnp.dot(xs[stage, m], wgu[j], preferred_element_type=jnp.float32)
            value = (jax.nn.gelu(both[:, :FT]) * both[:, FT:]).astype(jnp.bfloat16)
            h[stage, m, :, pl.ds(pl.multiple_of(j * FT, FT), FT)] = value

    def term(stage, which, t):
        return jnp.dot(h[stage, which], wds[t], preferred_element_type=jnp.float32)

    def down_for_partner(stage, which, src, slot):
        @pl.loop(0, n_nt)
        def _(t):
            src[:, cols(t)] = term(stage, which, t).astype(jnp.bfloat16)
            trade(slot, src, t).start()

    def chip_sum(stage, which, slot, t):
        trade(slot, spare, t).wait_recv()
        return term(stage, which, t) + rp[slot, :, cols(t)].astype(jnp.float32)

    spare = xs.at[NEAR, core]

    barrier = pltpu.get_barrier_semaphore()
    pl.semaphore_signal(barrier, inc=1, **to(behind))

    @pl.when(core == 1)
    def _():
        pl.semaphore_signal(barrier, inc=1, **to(partner))
        pl.semaphore_wait(barrier, 1)

    @pl.when(core == 0)
    def _():
        pl.semaphore_wait(barrier, 2)

    gather(NEAR, 0).start()
    load_x().start()

    @pl.when(core == 0)
    def _():
        pl.semaphore_signal(ready, inc=1, **to(partner))

    @pl.loop(0, n_ft)
    def _(j):
        load_w(j, 0).start()
        load_w(j, 1).start()

    @pl.loop(0, n_nt)
    def _(t):
        load_wd(t).start()

    @pl.when(core == 1)
    def _():
        pl.semaphore_wait(ready, 1)

    for i in range(2):
        share(OWN, i).start()
    share(OWN, 0).wait_recv()
    share(OWN, 1).wait_recv()
    gather(NEAR, 1).start()
    load_x().wait()
    up_stage(OWN)

    for i in range(2):
        gather(NEAR, i).wait_recv()
        gather(FAR, i).start()
        share(NEAR, i).start()
    for i in range(2):
        gather(LAST, i).start()
    for i in range(2):
        share(NEAR, i).wait_recv()
    for writer in (behind, beside):
        pl.semaphore_signal(credit, inc=1, **to(writer))
    up_stage(NEAR)

    @pl.loop(0, n_nt)
    def _(t):
        load_wd(t).wait()

    down_for_partner(NEAR, other, spare, 0)

    @pl.loop(0, n_nt)
    def _(t):
        stg[:, cols(t)] = chip_sum(NEAR, core, 0, t).astype(jnp.bfloat16)

    pl.semaphore_wait(credit, 2)
    for owner in range(2):
        near_sum(owner).start()

    for i in range(2):
        gather(FAR, i).wait_recv()
        share(FAR, i).start()
    for i in range(2):
        share(FAR, i).wait()
    up_stage(FAR)
    down_for_partner(FAR, core, xs.at[FAR, 0], 1)

    @pl.loop(0, n_nt)
    def _(t):
        xs[FAR, 1, :, cols(t)] = chip_sum(FAR, other, 1, t).astype(jnp.bfloat16)
        at_end(FAR_PARTS, t, lambda i: far_sum(i).start())

    for i in range(2):
        gather(LAST, i).wait_recv()
        share(LAST, i).start()
    for i in range(2):
        gather(LAST, i).wait_send()
        gather(NEAR, i).wait_send()
    for writer in (behind, beside):
        pl.semaphore_signal(late_credit, inc=1, **to(writer))
    for i in range(2):
        share(LAST, i).wait()
    up_stage(LAST)

    @pl.loop(0, n_nt)
    def _(t):
        trade(0, spare, t).wait_send()
        trade(1, xs.at[FAR, 0], t).wait_send()

    down_for_partner(LAST, other, xs.at[LAST, 0], 0)
    down_for_partner(OWN, other, spare, 1)
    pl.semaphore_wait(late_credit, 2)

    def send_last(i):
        for owner in range(2):
            last_sum(i, owner).start()

    @pl.loop(0, n_nt)
    def _(t):
        total = chip_sum(LAST, core, 0, t)
        at_start(FAR_PARTS, t, lambda i: far_sum(i).wait_recv())
        total = total + rf[:, cols(t)].astype(jnp.float32)
        xs[LAST, 1, :, cols(t)] = total.astype(jnp.bfloat16)
        at_end(LAST_PARTS, t, send_last)

    for sent in range(2):
        near_sum(core, sent).wait_recv()

    @pl.loop(0, n_nt)
    def _(t):
        trade(0, xs.at[LAST, 0], t).wait_send()
        trade(1, spare, t).wait_send()

    for i in range(2):
        gather(FAR, i).wait_send()
        share(OWN, i).wait_send()
        share(NEAR, i).wait_send()
        near_sum(i).wait_send()
    for i in range(len(FAR_PARTS)):
        far_sum(i).wait_send()

    def await_last(i):
        for owner in range(2):
            if i > 0:
                last_sum(i - 1, owner).wait_send()
        for sent in range(2):
            last_sum(i, core, sent).wait_recv()

    @pl.loop(0, n_nt)
    def _(t):
        total = chip_sum(OWN, core, 1, t) + xs[OWN, core, :, cols(t)].astype(jnp.float32)
        at_start(LAST_PARTS, t, await_last)
        total = total + xs[OWN, other, :, cols(t)].astype(jnp.float32)
        y[:, cols(t)] = total.astype(jnp.bfloat16)

    for owner in range(2):
        last_sum(len(LAST_PARTS) - 1, owner).wait_send()


def solution(mesh):
    n = mesh.shape["tp"]

    def step(x, w_gate, w_up, w_down):
        rows, depth = x.shape
        hidden = w_gate.shape[1]
        n_ft, n_nt = hidden // FT, depth // NT
        dma, plain = pltpu.SemaphoreType.DMA, pltpu.SemaphoreType.REGULAR
        any_space = pl.BlockSpec(memory_space=pl.ANY)
        return pl.pallas_call(
            functools.partial(kernel, n),
            out_shape=pltpu.VMEM((rows, depth), jnp.bfloat16),
            in_specs=[any_space] * 4,
            out_specs=pl.BlockSpec(memory_space=pltpu.VMEM),
            scratch_shapes=[
                pltpu.VMEM((4, 2, rows, depth), jnp.bfloat16),
                pltpu.VMEM((n_ft, depth, 2 * FT), jnp.bfloat16),
                pltpu.VMEM((n_nt, hidden, NT), jnp.bfloat16),
                pltpu.VMEM((4, 2, rows, hidden), jnp.bfloat16),
                pltpu.VMEM((2, rows, depth), jnp.bfloat16),
                pltpu.VMEM((rows, depth), jnp.bfloat16),
                pltpu.VMEM((rows, depth), jnp.bfloat16),
                dma((4, 2)),
                dma((4, 2)),
                dma((4, 2)),
                dma((4, 2)),
                dma((2, n_nt)),
                dma((2, n_nt)),
                dma((2,)),
                dma((2,)),
                dma((len(FAR_PARTS),)),
                dma((len(FAR_PARTS),)),
                dma((len(LAST_PARTS), 2)),
                dma((len(LAST_PARTS), 2)),
                dma((2, n_ft)),
                dma((n_nt,)),
                dma,
                plain,
                plain,
                plain,
            ],
            compiler_params=pltpu.CompilerParams(
                collective_id=0, has_side_effects=True, vmem_limit_bytes=61 * 2**20
            ),
            cost_estimate=pl.CostEstimate(
                flops=6 * n * rows * depth * hidden, bytes_accessed=6 * depth * hidden, transcendentals=0
            ),
        )(x, w_gate, w_up, w_down)

    return jax.shard_map(
        step,
        mesh=mesh,
        in_specs=(P(("dp", "tp"), None), P(None, "tp"), P(None, "tp"), P("tp", None)),
        out_specs=P(("dp", "tp"), None),
        check_vma=False,
    )
```

```python
import functools

import jax
import jax.numpy as jnp
from jax import lax
from jax.experimental import pallas as pl
from jax.experimental.pallas import tpu as pltpu
from jax.sharding import PartitionSpec as P

MESH = pl.DeviceIdType.MESH
FT = 256
NT = 512
FAR_PARTS = (4, 4)
TRADE_PARTS = (4, 4)
LAST_PARTS = (4, 3, 1)
OWN, NEAR, FAR, LAST = range(4)


def kernel(
    n, x, wg, wu, wd, y, xs, wgu, wds, h, rp, rf, stg,
    g_send, g_recv, d_send, d_recv, p_send, p_recv, n_send, n_recv, f_send, f_recv, l_send, l_recv,
    w_sem, wd_sem, x_sem, ready, credit, late_credit,
):
    rows, depth = x.shape
    hidden = wg.shape[1]
    half = rows // 2
    n_ft, n_nt = hidden // FT, depth // NT

    me = lax.axis_index("tp")
    core = lax.rem(me, 2)
    other = 1 - core
    way = other
    partner = me + 1 - 2 * core
    ahead = lax.rem(me + 4 * core - 2 + n, n)
    behind = lax.rem(me + 2 - 4 * core + n, n)
    beside = ahead + 1 - 2 * core

    def to(index):
        return dict(device_id={"tp": index}, device_id_type=MESH)

    def block(i):
        return pl.ds(pl.multiple_of(i * half, half), half)

    def cols(t, steps=1):
        return pl.ds(pl.multiple_of(t * NT, NT), steps * NT)

    def gather(stage, i):
        origin = (core, other)[i]
        part = block(1 - way if stage == LAST else way)
        src = xs.at[NEAR, way, block(origin)] if stage == FAR else (x.at[part], xs.at[OWN, other, part])[i]
        dst = xs.at[stage, way, block(origin)]
        return pltpu.make_async_remote_copy(src, dst, g_send.at[stage - 1], g_recv.at[stage - 1, i], **to(ahead))

    def gathered(stage):
        both = xs.at[stage, way]
        return pltpu.make_async_remote_copy(both, both, g_send.at[stage - 1], g_recv.at[stage - 1, 0], **to(ahead))

    def share(stage, i):
        if stage == OWN:
            part = block((core, other)[i])
            src, dst = x.at[part], xs.at[OWN, core, part]
        else:
            src = dst = xs.at[stage, way, block((core, other)[i])]
        return pltpu.make_async_remote_copy(src, dst, d_send.at[stage], d_recv.at[stage], **to(partner))

    def shared(stage):
        src, dst = (x, xs.at[OWN, core]) if stage == OWN else (xs.at[stage, way],) * 2
        return pltpu.make_async_remote_copy(src, dst, d_send.at[stage], d_recv.at[stage], **to(partner))

    def trade(slot, src, i):
        some = pl.ds(sum(TRADE_PARTS[:i]) * NT, TRADE_PARTS[i] * NT)
        return pltpu.make_async_remote_copy(
            src.at[:, some], rp.at[slot, :, some], p_send.at[slot], p_recv.at[slot, i], **to(partner)
        )

    def traded(slot, src):
        return pltpu.make_async_remote_copy(src, rp.at[slot], p_send.at[slot], p_recv.at[slot, 0], **to(partner))

    def near_sum(owner):
        dst = xs.at[OWN, owner, block(1 - way)]
        return pltpu.make_async_remote_copy(stg.at[block(owner)], dst, n_send, n_recv, **to(ahead - core + owner))

    def near_sums():
        return pltpu.make_async_remote_copy(stg, xs.at[OWN, core], n_send, n_recv, **to(ahead))

    def far_sum(i):
        some = pl.ds(sum(FAR_PARTS[:i]) * NT, FAR_PARTS[i] * NT)
        return pltpu.make_async_remote_copy(xs.at[FAR, 1, :, some], rf.at[:, some], f_send, f_recv.at[i], **to(ahead))

    def far_sums():
        return pltpu.make_async_remote_copy(xs.at[FAR, 1], rf, f_send, f_recv.at[0], **to(ahead))

    def last_sum(i, owner):
        some = pl.ds(sum(LAST_PARTS[:i]) * NT, LAST_PARTS[i] * NT)
        src, dst = xs.at[LAST, 1, block(owner), some], xs.at[OWN, 1 - owner, block(way), some]
        return pltpu.make_async_remote_copy(src, dst, l_send, l_recv.at[i], **to(ahead - core + owner))

    def last_sums(i=None):
        some = pl.ds(0, depth) if i is None else pl.ds(sum(LAST_PARTS[:i]) * NT, LAST_PARTS[i] * NT)
        src, dst = xs.at[LAST, 1, :, some], xs.at[OWN, other, :, some]
        return pltpu.make_async_remote_copy(src, dst, l_send, l_recv.at[i or 0], **to(ahead))

    def at_start(parts, t, act):
        for i in range(len(parts)):
            pl.when(t == sum(parts[:i]))(functools.partial(act, i))

    def at_end(parts, t, act):
        for i in range(len(parts)):
            pl.when(t == sum(parts[: i + 1]) - 1)(functools.partial(act, i))

    def load_x():
        return pltpu.make_async_copy(x, xs.at[OWN, core], x_sem)

    def load_w(j, which):
        src = (wg, wu)[which].at[:, pl.ds(pl.multiple_of(j * FT, FT), FT)]
        return pltpu.make_async_copy(src, wgu.at[j, :, pl.ds(which * FT, FT)], w_sem.at[j])

    def loaded_w(j):
        return pltpu.make_async_copy(wg.at[:, pl.ds(0, 2 * FT)], wgu.at[j], w_sem.at[j])

    def load_wd():
        return pltpu.make_async_copy(wd, wds, wd_sem)

    def up_stage(stage):
        @pl.loop(0, n_ft * 2)
        def _(i):
            j, m = i // 2, lax.rem(i, 2)
            if stage == OWN:

                @pl.when(m == 0)
                def _():
                    loaded_w(j).wait()

            both = jnp.dot(xs[stage, m], wgu[j], preferred_element_type=jnp.float32)
            value = (jax.nn.gelu(both[:, :FT]) * both[:, FT:]).astype(jnp.bfloat16)
            h[stage, m, :, pl.ds(pl.multiple_of(j * FT, FT), FT)] = value

    def term(stage, which, t):
        return jnp.dot(h[stage, which], wds[:, cols(t)], preferred_element_type=jnp.float32)

    def down_for_partner(stage, which, src, slot):
        @pl.loop(0, n_nt)
        def _(t):
            src[:, cols(t)] = term(stage, which, t).astype(jnp.bfloat16)
            at_end(TRADE_PARTS, t, lambda i: trade(slot, src, i).start())

    def chip_sum(stage, which, slot, t):
        at_start(TRADE_PARTS, t, lambda i: trade(slot, spare, i).wait_recv())
        return term(stage, which, t) + rp[slot, :, cols(t)].astype(jnp.float32)

    spare = xs.at[NEAR, core]

    barrier = pltpu.get_barrier_semaphore()
    pl.semaphore_signal(barrier, inc=1, **to(behind))

    @pl.when(core == 1)
    def _():
        pl.semaphore_signal(barrier, inc=1, **to(partner))
        pl.semaphore_wait(barrier, 1)

    @pl.when(core == 0)
    def _():
        pl.semaphore_wait(barrier, 2)

    gather(NEAR, 0).start()
    load_x().start()

    @pl.when(core == 0)
    def _():
        pl.semaphore_signal(ready, inc=1, **to(partner))

    @pl.loop(0, n_ft)
    def _(j):
        load_w(j, 0).start()
        load_w(j, 1).start()

    load_wd().start()

    @pl.when(core == 1)
    def _():
        pl.semaphore_wait(ready, 1)

    for i in range(2):
        share(OWN, i).start()
    shared(OWN).wait_recv()
    gather(NEAR, 1).start()
    load_x().wait()
    up_stage(OWN)

    for i in range(2):
        gather(NEAR, i).wait_recv()
        gather(FAR, i).start()
        share(NEAR, i).start()
    for i in range(2):
        gather(LAST, i).start()
    shared(NEAR).wait_recv()
    for writer in (behind, beside):
        pl.semaphore_signal(credit, inc=1, **to(writer))
    up_stage(NEAR)

    load_wd().wait()

    down_for_partner(NEAR, other, spare, 0)

    @pl.loop(0, n_nt)
    def _(t):
        stg[:, cols(t)] = chip_sum(NEAR, core, 0, t).astype(jnp.bfloat16)

    pl.semaphore_wait(credit, 2)
    for owner in range(2):
        near_sum(owner).start()

    for i in range(2):
        gather(FAR, i).wait_recv()
        share(FAR, i).start()
    shared(FAR).wait()
    up_stage(FAR)
    down_for_partner(FAR, core, xs.at[FAR, 0], 1)

    @pl.loop(0, n_nt)
    def _(t):
        xs[FAR, 1, :, cols(t)] = chip_sum(FAR, other, 1, t).astype(jnp.bfloat16)
        at_end(FAR_PARTS, t, lambda i: far_sum(i).start())

    for i in range(2):
        gather(LAST, i).wait_recv()
        share(LAST, i).start()
    gathered(LAST).wait_send()
    gathered(NEAR).wait_send()
    for writer in (behind, beside):
        pl.semaphore_signal(late_credit, inc=1, **to(writer))
    shared(LAST).wait()
    up_stage(LAST)

    traded(0, spare).wait_send()
    traded(1, xs.at[FAR, 0]).wait_send()

    down_for_partner(LAST, other, xs.at[LAST, 0], 0)
    down_for_partner(OWN, other, spare, 1)
    pl.semaphore_wait(late_credit, 2)

    def send_last(i):
        for owner in range(2):
            last_sum(i, owner).start()

    @pl.loop(0, n_nt)
    def _(t):
        total = chip_sum(LAST, core, 0, t)
        at_start(FAR_PARTS, t, lambda i: far_sum(i).wait_recv())
        total = total + rf[:, cols(t)].astype(jnp.float32)
        xs[LAST, 1, :, cols(t)] = total.astype(jnp.bfloat16)
        at_end(LAST_PARTS, t, send_last)

    near_sums().wait_recv()

    traded(0, xs.at[LAST, 0]).wait_send()
    traded(1, spare).wait_send()
    gathered(FAR).wait_send()
    shared(OWN).wait_send()
    shared(NEAR).wait_send()
    near_sums().wait_send()
    far_sums().wait_send()

    @pl.loop(0, n_nt)
    def _(t):
        total = chip_sum(OWN, core, 1, t) + xs[OWN, core, :, cols(t)].astype(jnp.float32)
        at_start(LAST_PARTS, t, lambda i: last_sums(i).wait_recv())
        total = total + xs[OWN, other, :, cols(t)].astype(jnp.float32)
        y[:, cols(t)] = total.astype(jnp.bfloat16)

    last_sums().wait_send()


def solution(mesh):
    n = mesh.shape["tp"]

    def step(x, w_gate, w_up, w_down):
        rows, depth = x.shape
        hidden = w_gate.shape[1]
        n_ft, n_nt = hidden // FT, depth // NT
        dma, plain = pltpu.SemaphoreType.DMA, pltpu.SemaphoreType.REGULAR
        any_space = pl.BlockSpec(memory_space=pl.ANY)
        return pl.pallas_call(
            functools.partial(kernel, n),
            out_shape=pltpu.VMEM((rows, depth), jnp.bfloat16),
            in_specs=[any_space] * 4,
            out_specs=pl.BlockSpec(memory_space=pltpu.VMEM),
            scratch_shapes=[
                pltpu.VMEM((4, 2, rows, depth), jnp.bfloat16),
                pltpu.VMEM((n_ft, depth, 2 * FT), jnp.bfloat16),
                pltpu.VMEM((hidden, depth), jnp.bfloat16),
                pltpu.VMEM((4, 2, rows, hidden), jnp.bfloat16),
                pltpu.VMEM((2, rows, depth), jnp.bfloat16),
                pltpu.VMEM((rows, depth), jnp.bfloat16),
                pltpu.VMEM((rows, depth), jnp.bfloat16),
                dma((3,)),
                dma((3, 2)),
                dma((4,)),
                dma((4,)),
                dma((2,)),
                dma((2, len(TRADE_PARTS))),
                dma,
                dma,
                dma,
                dma((len(FAR_PARTS),)),
                dma,
                dma((len(LAST_PARTS),)),
                dma((n_ft,)),
                dma,
                dma,
                plain,
                plain,
                plain,
            ],
            compiler_params=pltpu.CompilerParams(
                collective_id=0, has_side_effects=True, vmem_limit_bytes=61 * 2**20
            ),
            cost_estimate=pl.CostEstimate(
                flops=6 * n * rows * depth * hidden, bytes_accessed=6 * depth * hidden, transcendentals=0
            ),
        )(x, w_gate, w_up, w_down)

    return jax.shard_map(
        step,
        mesh=mesh,
        in_specs=(P(("dp", "tp"), None), P(None, "tp"), P(None, "tp"), P("tp", None)),
        out_specs=P(("dp", "tp"), None),
        check_vma=False,
    )
```

```python
import functools

import jax
import jax.numpy as jnp
from jax import lax
from jax.experimental import pallas as pl
from jax.experimental.pallas import tpu as pltpu
from jax.sharding import PartitionSpec as P

MESH = pl.DeviceIdType.MESH
FT = 256
NT = 512
FAR_PARTS = (4, 4)
TRADE_PARTS = (8,)
LAST_PARTS = (4, 3, 1)
OWN, NEAR, FAR, LAST = range(4)


def kernel(
    n, x, wg, wu, wd, y, xs, wgu, wds, h, rp, rf, stg,
    g_send, g_recv, d_send, d_recv, p_send, p_recv, s_send, n_recv, f_recv, l_recv,
    w_sem, wd_sem, x_sem, ready, credit, late_credit,
):
    rows, depth = x.shape
    hidden = wg.shape[1]
    half = rows // 2
    n_ft, n_nt = hidden // FT, depth // NT

    me = lax.axis_index("tp")
    core = lax.rem(me, 2)
    other = 1 - core
    way = other
    partner = me + 1 - 2 * core
    ahead = lax.rem(me + 4 * core - 2 + n, n)
    behind = lax.rem(me + 2 - 4 * core + n, n)
    beside = ahead + 1 - 2 * core

    def to(index):
        return dict(device_id={"tp": index}, device_id_type=MESH)

    def block(i):
        return pl.ds(pl.multiple_of(i * half, half), half)

    def cols(t, steps=1):
        return pl.ds(pl.multiple_of(t * NT, NT), steps * NT)

    def gather(stage, i):
        origin = (core, other)[i]
        part = block(1 - way if stage == LAST else way)
        src = xs.at[NEAR, way, block(origin)] if stage == FAR else (x.at[part], xs.at[OWN, other, part])[i]
        dst = xs.at[stage, way, block(origin)]
        return pltpu.make_async_remote_copy(src, dst, g_send, g_recv.at[i if stage == NEAR else stage], **to(ahead))

    def gathered(stage):
        both = xs.at[stage, way]
        return pltpu.make_async_remote_copy(both, both, g_send, g_recv.at[stage], **to(ahead))

    def all_out(sem):
        three = xs.at[pl.ds(NEAR, 3), 0]
        return pltpu.make_async_remote_copy(three, three, sem, g_recv.at[0], **to(ahead))

    def share(stage, i):
        if stage == OWN:
            part = block((core, other)[i])
            src, dst = x.at[part], xs.at[OWN, core, part]
        else:
            src = dst = xs.at[stage, way, block((core, other)[i])]
        return pltpu.make_async_remote_copy(src, dst, d_send.at[stage % 2], d_recv.at[stage % 2], **to(partner))

    def shared(stage):
        src, dst = (x, xs.at[OWN, core]) if stage == OWN else (xs.at[stage, way],) * 2
        return pltpu.make_async_remote_copy(src, dst, d_send.at[stage % 2], d_recv.at[stage % 2], **to(partner))

    def trade(slot, src, i):
        some = pl.ds(sum(TRADE_PARTS[:i]) * NT, TRADE_PARTS[i] * NT)
        return pltpu.make_async_remote_copy(
            src.at[:, some], rp.at[slot, :, some], p_send.at[slot], p_recv.at[slot, i], **to(partner)
        )

    def traded(slot, src):
        return pltpu.make_async_remote_copy(src, rp.at[slot], p_send.at[slot], p_recv.at[slot, 0], **to(partner))

    def near_sum(owner):
        dst = xs.at[OWN, owner, block(1 - way)]
        return pltpu.make_async_remote_copy(stg.at[block(owner)], dst, s_send, n_recv, **to(ahead - core + owner))

    def near_sums():
        return pltpu.make_async_remote_copy(stg, xs.at[OWN, core], s_send, n_recv, **to(ahead))

    def far_sum(i):
        some = pl.ds(sum(FAR_PARTS[:i]) * NT, FAR_PARTS[i] * NT)
        return pltpu.make_async_remote_copy(xs.at[FAR, 1, :, some], rf.at[:, some], s_send, f_recv.at[i], **to(ahead))

    def last_sum(i, owner):
        some = pl.ds(sum(LAST_PARTS[:i]) * NT, LAST_PARTS[i] * NT)
        src, dst = xs.at[LAST, 1, block(owner), some], xs.at[OWN, 1 - owner, block(way), some]
        return pltpu.make_async_remote_copy(src, dst, s_send, l_recv.at[i], **to(ahead - core + owner))

    def last_sums(i):
        some = pl.ds(sum(LAST_PARTS[:i]) * NT, LAST_PARTS[i] * NT)
        src, dst = xs.at[LAST, 1, :, some], xs.at[OWN, other, :, some]
        return pltpu.make_async_remote_copy(src, dst, s_send, l_recv.at[i], **to(ahead))

    def at_start(parts, t, act):
        for i in range(len(parts)):
            pl.when(t == sum(parts[:i]))(functools.partial(act, i))

    def at_end(parts, t, act):
        for i in range(len(parts)):
            pl.when(t == sum(parts[: i + 1]) - 1)(functools.partial(act, i))

    def load_x():
        return pltpu.make_async_copy(x, xs.at[OWN, core], x_sem)

    def load_w(j, which):
        src = (wg, wu)[which].at[:, pl.ds(pl.multiple_of(j * FT, FT), FT)]
        return pltpu.make_async_copy(src, wgu.at[j, :, pl.ds(which * FT, FT)], w_sem.at[j])

    def loaded_w(j):
        return pltpu.make_async_copy(wg.at[:, pl.ds(0, 2 * FT)], wgu.at[j], w_sem.at[j])

    def load_wd():
        return pltpu.make_async_copy(wd, wds, wd_sem)

    def up_stage(stage):
        @pl.loop(0, n_ft * 2)
        def _(i):
            j, m = i // 2, lax.rem(i, 2)
            if stage == OWN:

                @pl.when(m == 0)
                def _():
                    loaded_w(j).wait()

            both = jnp.dot(xs[stage, m], wgu[j], preferred_element_type=jnp.float32)
            value = (jax.nn.gelu(both[:, :FT]) * both[:, FT:]).astype(jnp.bfloat16)
            h[stage, m, :, pl.ds(pl.multiple_of(j * FT, FT), FT)] = value

    def term(stage, which, t):
        return jnp.dot(h[stage, which], wds[:, cols(t)], preferred_element_type=jnp.float32)

    def down_for_partner(stage, which, src, slot):
        @pl.loop(0, n_nt)
        def _(t):
            src[:, cols(t)] = term(stage, which, t).astype(jnp.bfloat16)
            at_end(TRADE_PARTS, t, lambda i: trade(slot, src, i).start())

    def chip_sum(stage, which, slot, t):
        at_start(TRADE_PARTS, t, lambda i: trade(slot, spare, i).wait_recv())
        return term(stage, which, t) + rp[slot, :, cols(t)].astype(jnp.float32)

    spare = xs.at[NEAR, core]

    barrier = pltpu.get_barrier_semaphore()
    pl.semaphore_signal(barrier, inc=1, **to(behind))

    @pl.when(core == 1)
    def _():
        pl.semaphore_signal(barrier, inc=1, **to(partner))
        pl.semaphore_wait(barrier, 1)

    @pl.when(core == 0)
    def _():
        pl.semaphore_wait(barrier, 2)

    gather(NEAR, 0).start()
    load_x().start()

    @pl.when(core == 0)
    def _():
        pl.semaphore_signal(ready, inc=1, **to(partner))

    @pl.loop(0, n_ft)
    def _(j):
        load_w(j, 0).start()
        load_w(j, 1).start()

    load_wd().start()

    @pl.when(core == 1)
    def _():
        pl.semaphore_wait(ready, 1)

    for i in range(2):
        share(OWN, i).start()
    shared(OWN).wait_recv()
    gather(NEAR, 1).start()
    load_x().wait()
    up_stage(OWN)

    for i in range(2):
        gather(NEAR, i).wait_recv()
        gather(FAR, i).start()
        share(NEAR, i).start()
    for i in range(2):
        gather(LAST, i).start()
    shared(NEAR).wait_recv()
    for writer in (behind, beside):
        pl.semaphore_signal(credit, inc=1, **to(writer))
    up_stage(NEAR)

    load_wd().wait()

    down_for_partner(NEAR, other, spare, 0)

    @pl.loop(0, n_nt)
    def _(t):
        stg[:, cols(t)] = chip_sum(NEAR, core, 0, t).astype(jnp.bfloat16)

    pl.semaphore_wait(credit, 2)
    for owner in range(2):
        near_sum(owner).start()

    gathered(FAR).wait_recv()
    shared(OWN).wait_send()
    shared(FAR).start()
    shared(FAR).wait()
    up_stage(FAR)
    down_for_partner(FAR, core, xs.at[FAR, 0], 1)

    @pl.loop(0, n_nt)
    def _(t):
        xs[FAR, 1, :, cols(t)] = chip_sum(FAR, other, 1, t).astype(jnp.bfloat16)
        at_end(FAR_PARTS, t, lambda i: far_sum(i).start())

    gathered(LAST).wait_recv()
    shared(NEAR).wait_send()
    shared(LAST).start()
    all_out(g_send).wait_send()
    for writer in (behind, beside):
        pl.semaphore_signal(late_credit, inc=1, **to(writer))
    shared(LAST).wait()
    up_stage(LAST)

    traded(0, spare).wait_send()
    traded(1, xs.at[FAR, 0]).wait_send()

    down_for_partner(LAST, other, xs.at[LAST, 0], 0)
    down_for_partner(OWN, other, spare, 1)
    pl.semaphore_wait(late_credit, 2)

    def send_last(i):
        for owner in range(2):
            last_sum(i, owner).start()

    @pl.loop(0, n_nt)
    def _(t):
        total = chip_sum(LAST, core, 0, t)
        at_start(FAR_PARTS, t, lambda i: far_sum(i).wait_recv())
        total = total + rf[:, cols(t)].astype(jnp.float32)
        xs[LAST, 1, :, cols(t)] = total.astype(jnp.bfloat16)
        at_end(LAST_PARTS, t, send_last)

    near_sums().wait_recv()

    traded(0, xs.at[LAST, 0]).wait_send()
    traded(1, spare).wait_send()

    @pl.loop(0, n_nt)
    def _(t):
        total = chip_sum(OWN, core, 1, t) + xs[OWN, core, :, cols(t)].astype(jnp.float32)
        at_start(LAST_PARTS, t, lambda i: last_sums(i).wait_recv())
        total = total + xs[OWN, other, :, cols(t)].astype(jnp.float32)
        y[:, cols(t)] = total.astype(jnp.bfloat16)

    all_out(s_send).wait_send()


def solution(mesh):
    n = mesh.shape["tp"]

    def step(x, w_gate, w_up, w_down):
        rows, depth = x.shape
        hidden = w_gate.shape[1]
        n_ft, n_nt = hidden // FT, depth // NT
        dma, plain = pltpu.SemaphoreType.DMA, pltpu.SemaphoreType.REGULAR
        any_space = pl.BlockSpec(memory_space=pl.ANY)
        return pl.pallas_call(
            functools.partial(kernel, n),
            out_shape=pltpu.VMEM((rows, depth), jnp.bfloat16),
            in_specs=[any_space] * 4,
            out_specs=pl.BlockSpec(memory_space=pltpu.VMEM),
            scratch_shapes=[
                pltpu.VMEM((4, 2, rows, depth), jnp.bfloat16),
                pltpu.VMEM((n_ft, depth, 2 * FT), jnp.bfloat16),
                pltpu.VMEM((hidden, depth), jnp.bfloat16),
                pltpu.VMEM((4, 2, rows, hidden), jnp.bfloat16),
                pltpu.VMEM((2, rows, depth), jnp.bfloat16),
                pltpu.VMEM((rows, depth), jnp.bfloat16),
                pltpu.VMEM((rows, depth), jnp.bfloat16),
                dma,
                dma((4,)),
                dma((2,)),
                dma((2,)),
                dma((2,)),
                dma((2, len(TRADE_PARTS))),
                dma,
                dma,
                dma((len(FAR_PARTS),)),
                dma((len(LAST_PARTS),)),
                dma((n_ft,)),
                dma,
                dma,
                plain,
                plain,
                plain,
            ],
            compiler_params=pltpu.CompilerParams(
                collective_id=0, has_side_effects=True, vmem_limit_bytes=61 * 2**20
            ),
            cost_estimate=pl.CostEstimate(
                flops=6 * n * rows * depth * hidden, bytes_accessed=6 * depth * hidden, transcendentals=0
            ),
        )(x, w_gate, w_up, w_down)

    return jax.shard_map(
        step,
        mesh=mesh,
        in_specs=(P(("dp", "tp"), None), P(None, "tp"), P(None, "tp"), P("tp", None)),
        out_specs=P(("dp", "tp"), None),
        check_vma=False,
    )
```

```python
import functools

import jax
import jax.numpy as jnp
from jax import lax
from jax.experimental import pallas as pl
from jax.experimental.pallas import tpu as pltpu
from jax.sharding import PartitionSpec as P

MESH = pl.DeviceIdType.MESH
FT = 256
NT = 512
FAR_PARTS = (4, 4)
TRADE_PARTS = (8,)
LAST_PARTS = (4, 3, 1)
OWN, NEAR, FAR, LAST = range(4)


def kernel(
    n, x, wg, wu, wd, y, xs, wgu, wds, h, rp, rf, stg,
    g_send, g_recv, d_send, d_recv, p_send, p_recv, s_send, n_recv, f_recv, l_recv,
    w_sem, wd_sem, ready, credit, late_credit,
):
    rows, depth = x.shape
    hidden = wg.shape[1]
    half = rows // 2
    n_ft, n_nt = hidden // FT, depth // NT

    me = lax.axis_index("tp")
    core = lax.rem(me, 2)
    other = 1 - core
    way = other
    partner = me + 1 - 2 * core
    ahead = lax.rem(me + 4 * core - 2 + n, n)
    behind = lax.rem(me + 2 - 4 * core + n, n)
    beside = ahead + 1 - 2 * core

    def to(index):
        return dict(device_id={"tp": index}, device_id_type=MESH)

    def block(i):
        return pl.ds(pl.multiple_of(i * half, half), half)

    def cols(t, steps=1):
        return pl.ds(pl.multiple_of(t * NT, NT), steps * NT)

    def gather(stage, i):
        origin = (core, other)[i]
        part = block(1 - way if stage == LAST else way)
        src = xs.at[NEAR, way, block(origin)] if stage == FAR else (x.at[part], xs.at[OWN, other, part])[i]
        dst = xs.at[stage, way, block(origin)]
        return pltpu.make_async_remote_copy(src, dst, g_send, g_recv.at[i if stage == NEAR else stage], **to(ahead))

    def gathered(stage):
        both = xs.at[stage, way]
        return pltpu.make_async_remote_copy(both, both, g_send, g_recv.at[stage], **to(ahead))

    def all_out(sem):
        three = xs.at[pl.ds(NEAR, 3), 0]
        return pltpu.make_async_remote_copy(three, three, sem, g_recv.at[0], **to(ahead))

    def share(stage, i):
        if stage == OWN:
            part = block((core, other)[i])
            src, dst = x.at[part], xs.at[OWN, core, part]
        else:
            src = dst = xs.at[stage, way, block((core, other)[i])]
        return pltpu.make_async_remote_copy(src, dst, d_send.at[stage % 2], d_recv.at[stage % 2], **to(partner))

    def shared(stage):
        src, dst = (x, xs.at[OWN, core]) if stage == OWN else (xs.at[stage, way],) * 2
        return pltpu.make_async_remote_copy(src, dst, d_send.at[stage % 2], d_recv.at[stage % 2], **to(partner))

    def trade(slot, src, i):
        some = pl.ds(sum(TRADE_PARTS[:i]) * NT, TRADE_PARTS[i] * NT)
        return pltpu.make_async_remote_copy(
            src.at[:, some], rp.at[slot, :, some], p_send.at[slot], p_recv.at[slot, i], **to(partner)
        )

    def traded(slot, src):
        return pltpu.make_async_remote_copy(src, rp.at[slot], p_send.at[slot], p_recv.at[slot, 0], **to(partner))

    def near_sum(owner):
        dst = xs.at[OWN, owner, block(1 - way)]
        return pltpu.make_async_remote_copy(stg.at[block(owner)], dst, s_send, n_recv, **to(ahead - core + owner))

    def near_sums():
        return pltpu.make_async_remote_copy(stg, xs.at[OWN, core], s_send, n_recv, **to(ahead))

    def far_sum(i):
        some = pl.ds(sum(FAR_PARTS[:i]) * NT, FAR_PARTS[i] * NT)
        return pltpu.make_async_remote_copy(xs.at[FAR, 1, :, some], rf.at[:, some], s_send, f_recv.at[i], **to(ahead))

    def last_sum(i, owner):
        some = pl.ds(sum(LAST_PARTS[:i]) * NT, LAST_PARTS[i] * NT)
        src, dst = xs.at[LAST, 1, block(owner), some], xs.at[OWN, 1 - owner, block(way), some]
        return pltpu.make_async_remote_copy(src, dst, s_send, l_recv.at[i], **to(ahead - core + owner))

    def last_sums(i):
        some = pl.ds(sum(LAST_PARTS[:i]) * NT, LAST_PARTS[i] * NT)
        src, dst = xs.at[LAST, 1, :, some], xs.at[OWN, other, :, some]
        return pltpu.make_async_remote_copy(src, dst, s_send, l_recv.at[i], **to(ahead))

    def at_start(parts, t, act):
        for i in range(len(parts)):
            pl.when(t == sum(parts[:i]))(functools.partial(act, i))

    def at_end(parts, t, act):
        for i in range(len(parts)):
            pl.when(t == sum(parts[: i + 1]) - 1)(functools.partial(act, i))

    def load_x():
        return pltpu.make_async_copy(x, xs.at[OWN, core], d_recv.at[OWN])

    def own_rows():
        both = xs.at[OWN]
        return pltpu.make_async_remote_copy(both, both, d_send.at[OWN], d_recv.at[OWN], **to(partner))

    def load_w(j, which):
        src = (wg, wu)[which].at[:, pl.ds(pl.multiple_of(j * FT, FT), FT)]
        return pltpu.make_async_copy(src, wgu.at[j, :, pl.ds(which * FT, FT)], w_sem.at[j])

    def loaded_w(j):
        return pltpu.make_async_copy(wg.at[:, pl.ds(0, 2 * FT)], wgu.at[j], w_sem.at[j])

    def load_wd():
        return pltpu.make_async_copy(wd, wds, wd_sem)

    def up_stage(stage):
        @pl.loop(0, n_ft * 2)
        def _(i):
            j, m = i // 2, lax.rem(i, 2)
            if stage == OWN:

                @pl.when(m == 0)
                def _():
                    loaded_w(j).wait()

            both = jnp.dot(xs[stage, m], wgu[j], preferred_element_type=jnp.float32)
            value = (jax.nn.gelu(both[:, :FT]) * both[:, FT:]).astype(jnp.bfloat16)
            h[stage, m, :, pl.ds(pl.multiple_of(j * FT, FT), FT)] = value

    def term(stage, which, t):
        return jnp.dot(h[stage, which], wds[:, cols(t)], preferred_element_type=jnp.float32)

    def down_for_partner(stage, which, src, slot):
        @pl.loop(0, n_nt)
        def _(t):
            src[:, cols(t)] = term(stage, which, t).astype(jnp.bfloat16)
            at_end(TRADE_PARTS, t, lambda i: trade(slot, src, i).start())

    def chip_sum(stage, which, slot, t):
        at_start(TRADE_PARTS, t, lambda i: trade(slot, spare, i).wait_recv())
        return term(stage, which, t) + rp[slot, :, cols(t)].astype(jnp.float32)

    spare = xs.at[NEAR, core]

    barrier = pltpu.get_barrier_semaphore()
    pl.semaphore_signal(barrier, inc=1, **to(behind))

    @pl.when(core == 1)
    def _():
        pl.semaphore_signal(barrier, inc=1, **to(partner))
        pl.semaphore_wait(barrier, 1)

    @pl.when(core == 0)
    def _():
        pl.semaphore_wait(barrier, 2)

    gather(NEAR, 0).start()
    load_x().start()

    @pl.when(core == 0)
    def _():
        pl.semaphore_signal(ready, inc=1, **to(partner))

    @pl.loop(0, n_ft)
    def _(j):
        load_w(j, 0).start()
        load_w(j, 1).start()

    load_wd().start()

    @pl.when(core == 1)
    def _():
        pl.semaphore_wait(ready, 1)

    for i in range(2):
        share(OWN, i).start()
    own_rows().wait_recv()
    gather(NEAR, 1).start()
    up_stage(OWN)

    for i in range(2):
        gather(NEAR, i).wait_recv()
        gather(FAR, i).start()
        share(NEAR, i).start()
    for i in range(2):
        gather(LAST, i).start()
    shared(NEAR).wait_recv()
    for writer in (behind, beside):
        pl.semaphore_signal(credit, inc=1, **to(writer))
    up_stage(NEAR)

    load_wd().wait()

    down_for_partner(NEAR, other, spare, 0)

    @pl.loop(0, n_nt)
    def _(t):
        stg[:, cols(t)] = chip_sum(NEAR, core, 0, t).astype(jnp.bfloat16)

    pl.semaphore_wait(credit, 2)
    for owner in range(2):
        near_sum(owner).start()

    gathered(FAR).wait_recv()
    shared(OWN).wait_send()
    shared(FAR).start()
    shared(FAR).wait()
    up_stage(FAR)
    down_for_partner(FAR, core, xs.at[FAR, 0], 1)

    @pl.loop(0, n_nt)
    def _(t):
        xs[FAR, 1, :, cols(t)] = chip_sum(FAR, other, 1, t).astype(jnp.bfloat16)
        at_end(FAR_PARTS, t, lambda i: far_sum(i).start())

    gathered(LAST).wait_recv()
    shared(NEAR).wait_send()
    shared(LAST).start()
    all_out(g_send).wait_send()
    for writer in (behind, beside):
        pl.semaphore_signal(late_credit, inc=1, **to(writer))
    shared(LAST).wait()
    up_stage(LAST)

    traded(0, spare).wait_send()
    traded(1, xs.at[FAR, 0]).wait_send()

    down_for_partner(LAST, other, xs.at[LAST, 0], 0)
    down_for_partner(OWN, other, spare, 1)
    pl.semaphore_wait(late_credit, 2)

    def send_last(i):
        for owner in range(2):
            last_sum(i, owner).start()

    @pl.loop(0, n_nt)
    def _(t):
        total = chip_sum(LAST, core, 0, t)
        at_start(FAR_PARTS, t, lambda i: far_sum(i).wait_recv())
        total = total + rf[:, cols(t)].astype(jnp.float32)
        xs[LAST, 1, :, cols(t)] = total.astype(jnp.bfloat16)
        at_end(LAST_PARTS, t, send_last)

    near_sums().wait_recv()

    traded(0, xs.at[LAST, 0]).wait_send()
    traded(1, spare).wait_send()

    @pl.loop(0, n_nt)
    def _(t):
        total = chip_sum(OWN, core, 1, t) + xs[OWN, core, :, cols(t)].astype(jnp.float32)
        at_start(LAST_PARTS, t, lambda i: last_sums(i).wait_recv())
        total = total + xs[OWN, other, :, cols(t)].astype(jnp.float32)
        y[:, cols(t)] = total.astype(jnp.bfloat16)

    all_out(s_send).wait_send()


def solution(mesh):
    n = mesh.shape["tp"]

    def step(x, w_gate, w_up, w_down):
        rows, depth = x.shape
        hidden = w_gate.shape[1]
        n_ft, n_nt = hidden // FT, depth // NT
        dma, plain = pltpu.SemaphoreType.DMA, pltpu.SemaphoreType.REGULAR
        any_space = pl.BlockSpec(memory_space=pl.ANY)
        return pl.pallas_call(
            functools.partial(kernel, n),
            out_shape=pltpu.VMEM((rows, depth), jnp.bfloat16),
            in_specs=[any_space] * 4,
            out_specs=pl.BlockSpec(memory_space=pltpu.VMEM),
            scratch_shapes=[
                pltpu.VMEM((4, 2, rows, depth), jnp.bfloat16),
                pltpu.VMEM((n_ft, depth, 2 * FT), jnp.bfloat16),
                pltpu.VMEM((hidden, depth), jnp.bfloat16),
                pltpu.VMEM((4, 2, rows, hidden), jnp.bfloat16),
                pltpu.VMEM((2, rows, depth), jnp.bfloat16),
                pltpu.VMEM((rows, depth), jnp.bfloat16),
                pltpu.VMEM((rows, depth), jnp.bfloat16),
                dma,
                dma((4,)),
                dma((2,)),
                dma((2,)),
                dma((2,)),
                dma((2, len(TRADE_PARTS))),
                dma,
                dma,
                dma((len(FAR_PARTS),)),
                dma((len(LAST_PARTS),)),
                dma((n_ft,)),
                dma,
                plain,
                plain,
                plain,
            ],
            compiler_params=pltpu.CompilerParams(
                collective_id=0, has_side_effects=True, vmem_limit_bytes=61 * 2**20
            ),
            cost_estimate=pl.CostEstimate(
                flops=6 * n * rows * depth * hidden, bytes_accessed=6 * depth * hidden, transcendentals=0
            ),
        )(x, w_gate, w_up, w_down)

    return jax.shard_map(
        step,
        mesh=mesh,
        in_specs=(P(("dp", "tp"), None), P(None, "tp"), P(None, "tp"), P("tp", None)),
        out_specs=P(("dp", "tp"), None),
        check_vma=False,
    )
```
